32 devices in a mesh: lat: 4 (over y, x), lon: 8 (over z, core).
Axes of the slice: x: 2, y: 2, z: 4, core: 2. Of those that a mesh axis runs over, the one named last changes fastest.
Arguments:
- adjoint_in: bfloat16 [8, 100, 8, 1024], P(None, None, 'lat', 'lon'), may hold values from -6 to 6
- state: bfloat16 [2, 8, 100, 8, 1024], P(None, None, None, 'lat', 'lon'), may hold values from 0.29882812 to 1
- inverses: bfloat16 [3, 8, 100, 100], replicated
- courant_lon: float32 [8, 1024], P('lat', 'lon'), may hold values from 0.1 to 0.4
- courant_lat: float32 [8, 1024], P('lat', 'lon'), may hold values from 0.1 to 0.4
- emission: float32 [100, 8, 1024], P(None, 'lat', 'lon'), may hold values from 0.02 to 0.2
- region_id: int32 [8, 1024], P('lat', 'lon'), may hold values from 0 to 31, as said below
- stiffness: int32 [8, 8, 1024], P(None, 'lat', 'lon'), may hold values from 1 to 3
Outputs:
- adjoint_out: bfloat16 [8, 100, 8, 1024], P(None, None, 'lat', 'lon')
- emission_grad: float32 [32, 100], P(('lat', 'lon'))
The draws below stay inside these ranges and needn't reach their ends.
Inputs may be any that keep to these rules, and one draw needn't show every extreme that they name: `region_id`: constant on aligned tiles of 2 x 2 columns.
All inputs are finite; a program needn't handle non-finite values.
Results may differ from the reference program's by a relative error of at most 0.0048.
Values sent between devices are 32-bit elements; how exact they have to be, the bound alone decides.
A program may use at most 64 MiB of HBM per device.

```python
import math
import jax
import jax.numpy as jnp
from jax import lax

SPEC = 100
LEV = 8
STEPS = 3
NWIN = 2
ADV = 2
CLAT = 2
CLON = 128
NLAT = 8
NLON = 1024
REGIONS = 32


def draw_inverses(key, part):
    key_diag = jax.random.fold_in(key, 11)
    key_off = jax.random.fold_in(key, 12)
    diag = jax.random.uniform(key_diag, (STEPS, LEV, SPEC), jnp.float32, 0.7, 1.2)
    off = jax.random.normal(key_off, (STEPS, LEV, SPEC, SPEC), jnp.float32) * 0.4 * SPEC ** (-0.5)
    eye = jnp.eye(SPEC, dtype=jnp.float32)
    return (off * (1.0 - eye) + diag[..., None] * eye).astype(jnp.bfloat16)


def draw_region_id(key, part):
    tiles = jax.random.randint(jax.random.fold_in(key, 21), (NLAT // 2, NLON // 2), 0, REGIONS)
    return jnp.repeat(jnp.repeat(tiles, 2, axis=0), 2, axis=1).astype(jnp.int32)


def draw_stiffness(key, part):
    tile_cols = CLON // 2
    caps = jax.random.randint(jax.random.fold_in(key, 31), (NLAT // CLAT, NLON // tile_cols), 1, STEPS + 1)
    caps = jnp.repeat(jnp.repeat(caps, CLAT, axis=0), tile_cols, axis=1)
    extra = jax.random.randint(jax.random.fold_in(key, 32), (LEV, NLAT, NLON), 0, STEPS)
    return (1 + extra % caps[None, :, :]).astype(jnp.int32)


def levels(own_key, dims, cuts, least, high):
    loudness = 1.0
    for position, blocks in cuts:
        heights = jax.random.uniform(jax.random.fold_in(jax.random.fold_in(own_key, 6), position), (blocks,), jnp.float32, least / len(cuts), high / len(cuts))
        loudness = loudness * jnp.repeat(jnp.exp(heights), dims[position] // blocks).reshape((-1,) + (1,) * (len(dims) - 1 - position))
    return loudness


def bell_draw(stream_key, shape, scale, reach, shards=(), held_as=jnp.bfloat16):
    level = levels(stream_key, shape, shards, -0.22, 0.18) if shards else 1.0
    values = jax.random.normal(stream_key, shape, jnp.float32) * scale * level
    return jnp.minimum(jnp.maximum(values, -reach), reach).astype(held_as)


def setup_inputs(seed: int = 0) -> dict:
    seeds = jax.random.split(jax.random.key(seed), 9)
    adjoint_in = bell_draw(seeds[0], (LEV, SPEC, NLAT, NLON), 1.0, 6.0, ((2, 4), (3, 8)))
    state = jnp.clip(jnp.exp(math.log(1.0) - 1.2078867 * jax.random.uniform(seeds[1], (NWIN, LEV, SPEC, NLAT, NLON), jnp.float32) ** levels(seeds[1], (NWIN, LEV, SPEC, NLAT, NLON), ((3, 4), (4, 8)), -0.2, 0.2)), 0.29882812, 1.0).astype(jnp.bfloat16)
    inverses = draw_inverses(jax.random.fold_in(seeds[8], 71), 0)
    courant_lon = jnp.clip(0.1 + 0.3 * jax.random.uniform(seeds[3], (NLAT, NLON), jnp.float32) ** levels(seeds[3], (NLAT, NLON), ((0, 4), (1, 8)), -0.2, 0.2), 0.1, 0.4)
    courant_lat = jnp.clip(0.1 + 0.3 * jax.random.uniform(seeds[4], (NLAT, NLON), jnp.float32) ** levels(seeds[4], (NLAT, NLON), ((0, 4), (1, 8)), -0.2, 0.2), 0.1, 0.4)
    emission = jnp.clip(jnp.exp(math.log(0.2) - 2.3025851 * jax.random.uniform(seeds[5], (SPEC, NLAT, NLON), jnp.float32) ** levels(seeds[5], (SPEC, NLAT, NLON), ((1, 4), (2, 8)), -0.2, 0.2)), 0.02, 0.2)
    region_id = draw_region_id(jax.random.fold_in(seeds[8], 71), 0)
    stiffness = draw_stiffness(jax.random.fold_in(seeds[8], 71), 0)
    return {"adjoint_in": adjoint_in, "state": state, "inverses": inverses, "courant_lon": courant_lon, "courant_lat": courant_lat, "emission": emission, "region_id": region_id, "stiffness": stiffness}


def transport(lam, clon, clat):
    right = jnp.roll(lam, -1, axis=2)
    down = jnp.concatenate([lam[:, 1:, :], jnp.zeros_like(lam[:, :1, :])], axis=1)
    return (1.0 - clon - clat) * lam + clat * down + clon * right


def chem_level(lam, factor, mats, klass):
    spec = lam.shape[0]
    flat = lam.reshape(spec, -1)
    yfac = factor.reshape(spec, -1).astype(jnp.float32)
    live = klass.reshape(1, -1)
    for s in reversed(range(STEPS)):
        amat = mats[s].T
        first = jnp.dot(amat, flat.astype(jnp.bfloat16), preferred_element_type=jnp.float32)
        second = jnp.dot(amat, (first * yfac).astype(jnp.bfloat16), preferred_element_type=jnp.float32)
        third = jnp.dot(amat, (second * yfac).astype(jnp.bfloat16), preferred_element_type=jnp.float32)
        cand = 0.4 * flat + 0.3 * first + 0.2 * second + 0.1 * third
        flat = jnp.where(live > s, cand, flat)
    return flat.reshape(lam.shape)


def reference(adjoint_in, state, inverses, courant_lon, courant_lat, emission, region_id, stiffness):
    lam = adjoint_in.astype(jnp.float32)
    surface = jnp.zeros(emission.shape, jnp.float32)
    mats_by_level = jnp.transpose(inverses, (1, 0, 2, 3))
    for window in reversed(range(NWIN)):
        def level_work(items):
            lam_l, factor_l, mats_l, klass_l = items
            for k in range(ADV):
                lam_l = transport(lam_l, courant_lon, courant_lat)
            return chem_level(lam_l, factor_l, mats_l, klass_l)

        lam = lax.map(level_work, (lam, state[window], mats_by_level, stiffness))
        surface = surface + lam[0]
    contrib = (surface * emission).reshape(emission.shape[0], -1).T
    grad = jax.ops.segment_sum(contrib, region_id.reshape(-1), num_segments=REGIONS)
    return lam.astype(jnp.bfloat16), grad.astype(jnp.float32)
```

```python
import functools

import jax
import jax.numpy as jnp
from jax import lax
from jax.experimental import pallas as pl
from jax.experimental.pallas import tpu as pltpu
from jax.sharding import PartitionSpec as P

MESH = pl.DeviceIdType.MESH
LP = 2


def kernel(
    n_lat, n_lon,
    adj_hbm, state_hbm, inv_hbm, clon_ref, clat_ref, em_ref, reg_ref, stiff_ref,
    out_hbm, grad_ref,
    adj, state, inv, mats, lam_a, lam_b, west1, west2, south1, south2, east1, east2,
    tmp, fin, outbuf, coef, part, inbox1, turn, inbox2,
    adj_sem, state_sem, inv_sem, out_sem, send_sem, recv_sem, s1, r1, s2, r2,
):
    lev, rows2, cols = adj.shape
    nwin = state.shape[0]
    steps = inv.shape[0]
    spec = rows2 // 2
    per = lev // LP
    units = nwin * per
    lat, lon = lax.axis_index("lat"), lax.axis_index("lon")
    north = jnp.maximum(lat - 1, 0)
    west = lax.rem(lon + n_lon - 1, n_lon)
    has_north = lat > 0
    has_south = lat < n_lat - 1

    loads = [pltpu.make_async_copy(adj_hbm, adj, adj_sem)]
    loads[0].start()
    inv_load = pltpu.make_async_copy(inv_hbm, inv, inv_sem)
    inv_load.start()
    state_loads = [
        pltpu.make_async_copy(state_hbm.at[w], state.at[w], state_sem.at[w]) for w in range(nwin)
    ]
    for w in reversed(range(nwin)):
        state_loads[w].start()

    barrier = pltpu.get_barrier_semaphore()
    for k in range(1, n_lon):
        pl.semaphore_signal(barrier, inc=1, device_id=(lat, lax.rem(lon + k, n_lon)), device_id_type=MESH)
    for k in range(1, n_lat):
        pl.semaphore_signal(barrier, inc=1, device_id=(lax.rem(lat + k, n_lat), lon), device_id_type=MESH)

    for r in range(2):
        clon, clat = clon_ref[r:r + 1, :], clat_ref[r:r + 1, :]
        coef[0, r] = jnp.broadcast_to(1.0 - clon - clat, (8, cols))
        coef[1, r] = jnp.broadcast_to(clat, (8, cols))
        coef[2, r] = jnp.broadcast_to(clon, (8, cols))

    lane = lax.broadcasted_iota(jnp.int32, (spec, cols), 1)

    def weights(r):
        return coef[0, r, 0:1, :], coef[1, r, 0:1, :], coef[2, r, 0:1, :]

    def remote(kind, src, dst, u, device):
        return pltpu.make_async_remote_copy(
            src_ref=src.at[u], dst_ref=dst.at[u],
            send_sem=send_sem.at[kind, u], recv_sem=recv_sem.at[kind, u],
            device_id=device, device_id_type=MESH,
        )

    def row_copy(kind, u):
        src, dst = ((lam_a, south1), (lam_b, south2))[kind]
        return remote(kind, src.at[0], dst, u, (north, lon))

    def col_copy(kind, u):
        src, dst = ((west1, east1), (west2, east2))[kind]
        return remote(kind + 2, src, dst, u, (lat, west))

    def pack(row0, row1):
        return jnp.where(lane == 0, row0, pltpu.roll(row1, 1, 1))

    def shift(row0, row1, edge):
        right0 = pltpu.roll(jnp.where(lane == 0, edge, row0), cols - 1, 1)
        right1 = pltpu.roll(jnp.where(lane == 0, pltpu.roll(edge, cols - 1, 1), row1), cols - 1, 1)
        return right0, right1

    def launch(u):
        @pl.when(has_north)
        def _():
            row_copy(0, u).start()
        for p in range(LP):
            west1[u, p] = pack(lam_a[0, u, p], lam_a[1, u, p])
        col_copy(0, u).start()

    def first_step(u):
        col_copy(0, u).wait_recv()
        c0, a0, o0 = weights(0)
        c1, a1, o1 = weights(1)
        for p in range(LP):
            row0, row1 = lam_a[0, u, p], lam_a[1, u, p]
            right0, right1 = shift(row0, row1, east1[u, p])
            lam_b[0, u, p] = c0 * row0 + a0 * row1 + o0 * right0
            lam_b[1, u, p] = c1 * row1 + o1 * right1

        @pl.when(has_north)
        def _():
            row_copy(1, u).start()

        @pl.when(has_south)
        def _():
            row_copy(0, u).wait_recv()
        for p in range(LP):
            row1 = lam_b[1, u, p] + a1 * south1[u, p]
            lam_b[1, u, p] = row1
            west2[u, p] = pack(lam_b[0, u, p], row1)
        col_copy(1, u).start()

    def second_step(u):
        col_copy(1, u).wait_recv()

        @pl.when(has_south)
        def _():
            row_copy(1, u).wait_recv()
        c0, a0, o0 = weights(0)
        c1, a1, o1 = weights(1)
        window = nwin - 1 - u // per
        group = u % per
        flats, ys, lives = [], [], []
        for p in range(LP):
            level = group * LP + p
            row0, row1 = lam_b[0, u, p], lam_b[1, u, p]
            right0, right1 = shift(row0, row1, east2[u, p])
            new0 = c0 * row0 + a0 * row1 + o0 * right0
            new1 = c1 * row1 + a1 * south2[u, p] + o1 * right1
            flats.append(jnp.concatenate([new0, new1], axis=1))
            tmp[p] = state[window, level].astype(jnp.float32)
            ys.append(jnp.concatenate(
                [tmp[p, pl.ds(0, spec, stride=2), :], tmp[p, pl.ds(1, spec, stride=2), :]], axis=1))
            live = stiff_ref[level]
            lives.append(jnp.concatenate([live[0:1], live[1:2]], axis=1))
        for s in reversed(range(steps)):
            mat = [mats[s, group * LP + p] for p in range(LP)]
            v1 = [jnp.dot(mat[p], flats[p].astype(jnp.bfloat16), preferred_element_type=jnp.float32) for p in range(LP)]
            v2 = [jnp.dot(mat[p], (v1[p] * ys[p]).astype(jnp.bfloat16), preferred_element_type=jnp.float32) for p in range(LP)]
            v3 = [jnp.dot(mat[p], (v2[p] * ys[p]).astype(jnp.bfloat16), preferred_element_type=jnp.float32) for p in range(LP)]
            flats = [
                jnp.where(lives[p] > s, 0.4 * flats[p] + 0.3 * v1[p] + 0.2 * v2[p] + 0.1 * v3[p], flats[p])
                for p in range(LP)
            ]
        return flats

    def store(u, flats):
        @pl.when(u < units - per)
        def _():
            for p in range(LP):
                for r in range(2):
                    lam_a[r, u + per, p] = flats[p][:, r * cols:(r + 1) * cols]
            launch(u + per)

        @pl.when(u >= units - per)
        def _():
            group = u - (units - per)
            for p in range(LP):
                for r in range(2):
                    tmp[p, pl.ds(r, spec, stride=2), :] = flats[p][:, r * cols:(r + 1) * cols]
                outbuf[group, p] = tmp[p].astype(jnp.bfloat16)
            pltpu.make_async_copy(outbuf.at[group], out_hbm.at[group], out_sem.at[group]).start()

    def spread(k):
        to = lax.rem(lon + k, n_lon)
        return pltpu.make_async_remote_copy(
            src_ref=part.at[to], dst_ref=inbox1.at[lon], send_sem=s1.at[k], recv_sem=r1.at[lon],
            device_id=(lat, to), device_id_type=MESH)

    def spread_in(k):
        source = lax.rem(lon + k, n_lon)
        return source, pltpu.make_async_remote_copy(
            src_ref=part.at[source], dst_ref=inbox1.at[source], send_sem=s1.at[k], recv_sem=r1.at[source],
            device_id=(lat, source), device_id_type=MESH)

    def spread2(k):
        to = lax.rem(lat + k, n_lat)
        return pltpu.make_async_remote_copy(
            src_ref=turn.at[to], dst_ref=inbox2.at[lat], send_sem=s2.at[k], recv_sem=r2.at[lat],
            device_id=(to, lon), device_id_type=MESH)

    def spread2_in(k):
        source = lax.rem(lat + k, n_lat)
        return source, pltpu.make_async_remote_copy(
            src_ref=turn.at[source], dst_ref=inbox2.at[source], send_sem=s2.at[k], recv_sem=r2.at[source],
            device_id=(source, lon), device_id_type=MESH)

    def regions():
        lat8 = part.shape[1]
        contrib = jnp.concatenate([
            em_ref[pl.ds(r, spec, stride=2), :]
            * (lam_a[r, units - per, 0] + fin[:, r * cols:(r + 1) * cols])
            for r in range(2)], axis=1)
        where_from = jnp.concatenate([reg_ref[0:1, :], reg_ref[1:2, :]], axis=1)
        shape = (n_lon * lat8, 2 * cols)
        column = jnp.concatenate([jnp.full((lat8, 2 * cols), c, jnp.int32) for c in range(n_lon)], axis=0)
        band = lax.broadcasted_iota(jnp.int32, (lat8, 2 * cols), 0)
        band = jnp.concatenate([band] * n_lon, axis=0)
        onehot = (jnp.broadcast_to(where_from, shape) == band * n_lon + column).astype(jnp.float32)
        sums = lax.dot_general(
            onehot, contrib, (((1,), (1,)), ((), ())),
            precision=lax.Precision.HIGHEST, preferred_element_type=jnp.float32)
        for c in range(n_lon):
            part[c] = sums[c * lat8:(c + 1) * lat8]
        for k in range(1, n_lon):
            spread(k).start()

    def regions_turn():
        total = part[lon]
        for k in range(1, n_lon):
            source, copy = spread_in(k)
            copy.wait_recv()
            total = total + inbox1[source]
        for b in range(n_lat):
            turn[b] = total[b:b + 1]
        for k in range(1, n_lat):
            spread2(k).start()

    def regions_end():
        total = turn[lat]
        for k in range(1, n_lat):
            source, copy = spread2_in(k)
            copy.wait_recv()
            total = total + inbox2[source]
        grad_ref[...] = total

    @pl.when(jnp.logical_not(has_south))
    def _():
        south1[...] = jnp.zeros_like(south1)
        south2[...] = jnp.zeros_like(south2)

    loads[0].wait()
    for level in range(lev):
        p = level % LP
        tmp[p] = adj[level].astype(jnp.float32)
        for r in range(2):
            lam_a[r, level // LP, p] = tmp[p, pl.ds(r, spec, stride=2), :]

    pl.semaphore_wait(barrier, n_lon - 1 + n_lat - 1)
    launch(0)
    launch(1)
    inv_load.wait()
    for s in range(steps):
        for level in range(lev):
            mats[s, level] = inv[s, level].astype(jnp.float32).T.astype(jnp.bfloat16)
    first_step(0)
    for w in range(nwin):
        state_loads[w].wait()

    def body(u, carry):
        @pl.when(u + 2 < per)
        def _():
            launch(u + 2)

        @pl.when(u + 1 < units)
        def _():
            first_step(u + 1)
        flats = second_step(u)
        store(u, flats)

        @pl.when(u == units - per)
        def _():
            fin[...] = flats[0]
            regions()

        @pl.when(u == units - per + 2)
        def _():
            regions_turn()
        return carry

    lax.fori_loop(0, units, body, 0)
    regions_end()

    def drain(u, carry):
        @pl.when(has_north)
        def _():
            row_copy(0, u).wait_send()
            row_copy(1, u).wait_send()
        col_copy(0, u).wait_send()
        col_copy(1, u).wait_send()
        return carry

    lax.fori_loop(0, units, drain, 0)
    for k in range(1, n_lon):
        spread(k).wait_send()
    for k in range(1, n_lat):
        spread2(k).wait_send()
    for g in range(per):
        pltpu.make_async_copy(outbuf.at[g], out_hbm.at[g], out_sem.at[g]).wait()


def solution(mesh):
    n_lat, n_lon = mesh.shape["lat"], mesh.shape["lon"]

    def per_device(adjoint_in, state, inverses, courant_lon, courant_lat, emission, region_id, stiffness):
        lev, spec, rows, cols = adjoint_in.shape
        nwin, steps = state.shape[0], inverses.shape[0]
        per = lev // LP
        units = nwin * per
        lat8 = -(-n_lat // 8) * 8
        f32, bf16 = jnp.float32, jnp.bfloat16
        any_space = pl.BlockSpec(memory_space=pl.ANY)
        vmem = pl.BlockSpec(memory_space=pltpu.VMEM)
        halo = pltpu.VMEM((units, LP, spec, cols), f32)
        held = pltpu.VMEM((2, units, LP, spec, cols), f32)
        dma = pltpu.SemaphoreType.DMA
        out, grad = pl.pallas_call(
            functools.partial(kernel, n_lat, n_lon),
            out_shape=(
                jax.ShapeDtypeStruct((per, LP, rows * spec, cols), bf16),
                jax.ShapeDtypeStruct((1, spec), f32),
            ),
            in_specs=[any_space] * 3 + [vmem] * 5,
            out_specs=(any_space, vmem),
            scratch_shapes=[
                pltpu.VMEM((lev, rows * spec, cols), bf16),
                pltpu.VMEM((nwin, lev, rows * spec, cols), bf16),
                pltpu.VMEM(inverses.shape, bf16),
                pltpu.VMEM(inverses.shape, bf16),
                held, held, halo, halo, halo, halo, halo, halo,
                pltpu.VMEM((LP, rows * spec, cols), f32),
                pltpu.VMEM((spec, rows * cols), f32),
                pltpu.VMEM((per, LP, rows * spec, cols), bf16),
                pltpu.VMEM((3, rows, 8, cols), f32),
                pltpu.VMEM((n_lon, lat8, spec), f32),
                pltpu.VMEM((n_lon, lat8, spec), f32),
                pltpu.VMEM((n_lat, 1, spec), f32),
                pltpu.VMEM((n_lat, 1, spec), f32),
                dma, dma((nwin,)), dma, dma((per,)),
                dma((4, units)), dma((4, units)),
                dma((n_lon,)), dma((n_lon,)), dma((n_lat,)), dma((n_lat,)),
            ],
            compiler_params=pltpu.CompilerParams(collective_id=0, has_side_effects=True),
        )(
            adjoint_in.reshape(lev, spec * rows, cols),
            state.reshape(nwin, lev, spec * rows, cols),
            inverses, courant_lon, courant_lat,
            emission.reshape(spec * rows, cols), region_id, stiffness,
        )
        return out.reshape(adjoint_in.shape), grad

    in_specs = (
        P(None, None, "lat", "lon"),
        P(None, None, None, "lat", "lon"),
        P(),
        P("lat", "lon"),
        P("lat", "lon"),
        P(None, "lat", "lon"),
        P("lat", "lon"),
        P(None, "lat", "lon"),
    )
    out_specs = (P(None, None, "lat", "lon"), P(("lat", "lon"), None))
    return jax.shard_map(
        per_device, mesh=mesh, in_specs=in_specs, out_specs=out_specs, check_vma=False
    )
```

```python
import functools

import jax
import jax.numpy as jnp
from jax import lax
from jax.experimental import pallas as pl
from jax.experimental.pallas import tpu as pltpu
from jax.sharding import PartitionSpec as P

MESH = pl.DeviceIdType.MESH
LP = 2
AHEAD = 2


def kernel(
    n_lat, n_lon,
    adj_hbm, state_hbm, inv_hbm, clon_hbm, clat_hbm, em_hbm, reg_hbm, stiff_hbm,
    outbuf, grad_ref,
    adj, state, inv, clon_ref, clat_ref, em_ref, reg_ref, stiff_ref, tall, mats, lam_a, lam_b, west1, west2, south1, south2, east1, east2,
    tmp, fin, coef, part, inbox1, turn, inbox2,
    adj_sem, state_sem, inv_sem, small_sem, send_sem, recv_sem, s1, r1, s2, r2,
):
    lev, rows2, cols = adj.shape
    nwin = state.shape[0]
    steps = inv.shape[0]
    spec = rows2 // 2
    per = lev // LP
    units = nwin * per
    lat, lon = lax.axis_index("lat"), lax.axis_index("lon")
    north = jnp.maximum(lat - 1, 0)
    west = lax.rem(lon + n_lon - 1, n_lon)
    has_north = lat > 0
    has_south = lat < n_lat - 1

    barrier = pltpu.get_barrier_semaphore()
    for k in range(1, n_lon):
        pl.semaphore_signal(barrier, inc=1, device_id=(lat, lax.rem(lon + k, n_lon)), device_id_type=MESH)
    for k in range(1, n_lat):
        pl.semaphore_signal(barrier, inc=1, device_id=(lax.rem(lat + k, n_lat), lon), device_id_type=MESH)

    adj_loads = [
        pltpu.make_async_copy(
            adj_hbm.at[pl.ds(u * LP, LP)], adj.at[pl.ds(u * LP, LP)], adj_sem.at[u])
        for u in range(per)
    ]
    for load in adj_loads:
        load.start()
    inv_load = pltpu.make_async_copy(inv_hbm, inv, inv_sem)
    inv_load.start()
    small = [
        pltpu.make_async_copy(src, dst, small_sem.at[n])
        for n, (src, dst) in enumerate((
            (clon_hbm, clon_ref), (clat_hbm, clat_ref), (stiff_hbm, stiff_ref),
            (reg_hbm, reg_ref), (em_hbm, em_ref)))
    ]
    for load in small:
        load.start()
    state_loads = [
        pltpu.make_async_copy(state_hbm.at[w], state.at[w], state_sem.at[w]) for w in range(nwin)
    ]
    for w in reversed(range(nwin)):
        state_loads[w].start()

    lane = lax.broadcasted_iota(jnp.int32, (spec, cols), 1)

    def weights(r):
        return coef[0, r, 0:1, :], coef[1, r, 0:1, :], coef[2, r, 0:1, :]

    def remote(kind, src, dst, u, device):
        return pltpu.make_async_remote_copy(
            src_ref=src.at[u], dst_ref=dst.at[u],
            send_sem=send_sem.at[kind, u], recv_sem=recv_sem.at[kind, u],
            device_id=device, device_id_type=MESH,
        )

    def row_copy(kind, u):
        src, dst = ((lam_a, south1), (lam_b, south2))[kind]
        return remote(kind, src.at[0], dst, u, (north, lon))

    def col_copy(kind, u):
        src, dst = ((west1, east1), (west2, east2))[kind]
        return remote(kind + 2, src, dst, u, (lat, west))

    def pack(row0, row1):
        return jnp.where(lane == 0, row0, pltpu.roll(row1, 1, 1))

    def shift(row0, row1, edge):
        right0 = pltpu.roll(jnp.where(lane == 0, edge, row0), cols - 1, 1)
        right1 = pltpu.roll(jnp.where(lane == 0, pltpu.roll(edge, cols - 1, 1), row1), cols - 1, 1)
        return right0, right1

    def launch(u):
        @pl.when(has_north)
        def _():
            row_copy(0, u).start()
        for p in range(LP):
            west1[u, p] = pack(lam_a[0, u, p], lam_a[1, u, p])
        col_copy(0, u).start()

    def first_step(u):
        col_copy(0, u).wait_recv()
        c0, a0, o0 = weights(0)
        c1, a1, o1 = weights(1)
        for p in range(LP):
            row0, row1 = lam_a[0, u, p], lam_a[1, u, p]
            right0, right1 = shift(row0, row1, east1[u, p])
            lam_b[0, u, p] = c0 * row0 + a0 * row1 + o0 * right0
            lam_b[1, u, p] = c1 * row1 + o1 * right1

        @pl.when(has_north)
        def _():
            row_copy(1, u).start()

        @pl.when(has_south)
        def _():
            row_copy(0, u).wait_recv()
        for p in range(LP):
            row1 = lam_b[1, u, p] + a1 * south1[u, p]
            lam_b[1, u, p] = row1
            west2[u, p] = pack(lam_b[0, u, p], row1)
        col_copy(1, u).start()

    def second_step(u):
        col_copy(1, u).wait_recv()

        @pl.when(has_south)
        def _():
            row_copy(1, u).wait_recv()
        c0, a0, o0 = weights(0)
        c1, a1, o1 = weights(1)
        window = nwin - 1 - u // per
        group = u % per
        flats, ys, lives = [], [], []
        for p in range(LP):
            level = group * LP + p
            row0, row1 = lam_b[0, u, p], lam_b[1, u, p]
            right0, right1 = shift(row0, row1, east2[u, p])
            new0 = c0 * row0 + a0 * row1 + o0 * right0
            new1 = c1 * row1 + a1 * south2[u, p] + o1 * right1
            flats.append(jnp.concatenate([new0, new1], axis=1))
            tmp[p] = state[window, level].astype(jnp.float32)
            ys.append(jnp.concatenate(
                [tmp[p, pl.ds(0, spec, stride=2), :], tmp[p, pl.ds(1, spec, stride=2), :]], axis=1))
            live = stiff_ref[level]
            lives.append(jnp.concatenate([live[0:1], live[1:2]], axis=1))
        for s in reversed(range(steps)):
            mat = [mats[s, group * LP + p] for p in range(LP)]
            v1 = [jnp.dot(mat[p], flats[p].astype(jnp.bfloat16), preferred_element_type=jnp.float32) for p in range(LP)]
            v2 = [jnp.dot(mat[p], (v1[p] * ys[p]).astype(jnp.bfloat16), preferred_element_type=jnp.float32) for p in range(LP)]
            v3 = [jnp.dot(mat[p], (v2[p] * ys[p]).astype(jnp.bfloat16), preferred_element_type=jnp.float32) for p in range(LP)]
            flats = [
                jnp.where(lives[p] > s, 0.4 * flats[p] + 0.3 * v1[p] + 0.2 * v2[p] + 0.1 * v3[p], flats[p])
                for p in range(LP)
            ]
        return flats

    def store(u, flats):
        @pl.when(u < units - per)
        def _():
            for p in range(LP):
                for r in range(2):
                    lam_a[r, u + per, p] = flats[p][:, r * cols:(r + 1) * cols]
            launch(u + per)

        @pl.when(u >= units - per)
        def _():
            group = u - (units - per)
            for p in range(LP):
                for r in range(2):
                    tmp[p, pl.ds(r, spec, stride=2), :] = flats[p][:, r * cols:(r + 1) * cols]
                outbuf[group, p] = tmp[p].astype(jnp.bfloat16)

    def spread(k):
        to = lax.rem(lon + k, n_lon)
        return pltpu.make_async_remote_copy(
            src_ref=part.at[to], dst_ref=inbox1.at[lon], send_sem=s1.at[k], recv_sem=r1.at[lon],
            device_id=(lat, to), device_id_type=MESH)

    def spread_in(k):
        source = lax.rem(lon + k, n_lon)
        return source, pltpu.make_async_remote_copy(
            src_ref=part.at[source], dst_ref=inbox1.at[source], send_sem=s1.at[k], recv_sem=r1.at[source],
            device_id=(lat, source), device_id_type=MESH)

    def spread2(k):
        to = lax.rem(lat + k, n_lat)
        return pltpu.make_async_remote_copy(
            src_ref=turn.at[to], dst_ref=inbox2.at[lat], send_sem=s2.at[k], recv_sem=r2.at[lat],
            device_id=(to, lon), device_id_type=MESH)

    def spread2_in(k):
        source = lax.rem(lat + k, n_lat)
        return source, pltpu.make_async_remote_copy(
            src_ref=turn.at[source], dst_ref=inbox2.at[source], send_sem=s2.at[k], recv_sem=r2.at[source],
            device_id=(source, lon), device_id_type=MESH)

    def regions():
        lat8 = part.shape[1]
        contrib = jnp.concatenate([
            em_ref[pl.ds(r, spec, stride=2), :]
            * (lam_a[r, units - per, 0] + fin[:, r * cols:(r + 1) * cols])
            for r in range(2)], axis=1)
        where_from = jnp.concatenate([reg_ref[0:1, :], reg_ref[1:2, :]], axis=1)
        shape = (n_lon * lat8, 2 * cols)
        column = jnp.concatenate([jnp.full((lat8, 2 * cols), c, jnp.int32) for c in range(n_lon)], axis=0)
        band = lax.broadcasted_iota(jnp.int32, (lat8, 2 * cols), 0)
        band = jnp.concatenate([band] * n_lon, axis=0)
        onehot = (jnp.broadcast_to(where_from, shape) == band * n_lon + column).astype(jnp.float32)
        sums = lax.dot_general(
            onehot, contrib, (((1,), (1,)), ((), ())),
            precision=lax.Precision.HIGHEST, preferred_element_type=jnp.float32)
        for c in range(n_lon):
            part[c] = sums[c * lat8:(c + 1) * lat8]
        for k in range(1, n_lon):
            spread(k).start()

    def regions_turn():
        total = part[lon]
        for k in range(1, n_lon):
            source, copy = spread_in(k)
            copy.wait_recv()
            total = total + inbox1[source]
        for b in range(n_lat):
            turn[b] = total[b:b + 1]
        for k in range(1, n_lat):
            spread2(k).start()

    def regions_end():
        total = turn[lat]
        for k in range(1, n_lat):
            source, copy = spread2_in(k)
            copy.wait_recv()
            total = total + inbox2[source]
        grad_ref[...] = total

    def take(u):
        adj_loads[u].wait()
        for p in range(LP):
            tmp[p] = adj[u * LP + p].astype(jnp.float32)
            for r in range(2):
                lam_a[r, u, p] = tmp[p, pl.ds(r, spec, stride=2), :]

    take(0)
    pl.semaphore_wait(barrier, n_lon - 1 + n_lat - 1)
    launch(0)
    for u in range(1, AHEAD + 1):
        take(u)
        launch(u)

    @pl.when(jnp.logical_not(has_south))
    def _():
        south1[...] = jnp.zeros_like(south1)
        south2[...] = jnp.zeros_like(south2)

    for load in small:
        load.wait()
    for r in range(2):
        clon, clat = clon_ref[r:r + 1, :], clat_ref[r:r + 1, :]
        coef[0, r] = jnp.broadcast_to(1.0 - clon - clat, (8, cols))
        coef[1, r] = jnp.broadcast_to(clat, (8, cols))
        coef[2, r] = jnp.broadcast_to(clon, (8, cols))

    first_step(0)
    for u in range(AHEAD + 1, per):
        take(u)
    inv_load.wait()
    for s in range(steps):
        tall[...] = inv[s].astype(jnp.float32)
        for level in range(lev):
            mats[s, level] = tall[pl.ds(level, spec, stride=lev), :].T.astype(jnp.bfloat16)
    for u in range(1, AHEAD):
        first_step(u)
    for w in range(nwin):
        state_loads[w].wait()

    def body(u, carry):
        @pl.when(u + AHEAD + 1 < per)
        def _():
            launch(u + AHEAD + 1)

        @pl.when(u + AHEAD < units)
        def _():
            first_step(u + AHEAD)
        flats = second_step(u)
        store(u, flats)

        @pl.when(u == units - per)
        def _():
            fin[...] = flats[0]
            regions()

        @pl.when(u == units - per + 4 // LP)
        def _():
            regions_turn()
        return carry

    lax.fori_loop(0, units, body, 0)
    regions_end()

    def drain(u, carry):
        @pl.when(has_north)
        def _():
            row_copy(0, u).wait_send()
            row_copy(1, u).wait_send()
        col_copy(0, u).wait_send()
        col_copy(1, u).wait_send()
        return carry

    lax.fori_loop(0, units, drain, 0)
    for k in range(1, n_lon):
        spread(k).wait_send()
    for k in range(1, n_lat):
        spread2(k).wait_send()


def finish(held_ref, grad_ref, out_hbm, grad_hbm, sems):
    copies = [
        pltpu.make_async_copy(held_ref, out_hbm, sems.at[0]),
        pltpu.make_async_copy(grad_ref, grad_hbm, sems.at[1]),
    ]
    for copy in copies:
        copy.start()
    for copy in copies:
        copy.wait()


def solution(mesh):
    n_lat, n_lon = mesh.shape["lat"], mesh.shape["lon"]

    def per_device(adjoint_in, state, inverses, courant_lon, courant_lat, emission, region_id, stiffness):
        lev, spec, rows, cols = adjoint_in.shape
        nwin, steps = state.shape[0], inverses.shape[0]
        per = lev // LP
        units = nwin * per
        lat8 = -(-n_lat // 8) * 8
        f32, bf16 = jnp.float32, jnp.bfloat16
        any_space = pl.BlockSpec(memory_space=pl.ANY)
        vmem = pl.BlockSpec(memory_space=pltpu.VMEM)
        halo = pltpu.VMEM((units, LP, spec, cols), f32)
        held = pltpu.VMEM((2, units, LP, spec, cols), f32)
        dma = pltpu.SemaphoreType.DMA
        out, grad = pl.pallas_call(
            functools.partial(kernel, n_lat, n_lon),
            out_shape=(
                pltpu.VMEM((per, LP, rows * spec, cols), bf16),
                pltpu.VMEM((1, spec), f32),
            ),
            in_specs=[any_space] * 8,
            out_specs=(vmem, vmem),
            scratch_shapes=[
                pltpu.VMEM((lev, rows * spec, cols), bf16),
                pltpu.VMEM((nwin, lev, rows * spec, cols), bf16),
                pltpu.VMEM((steps, spec * lev, spec), bf16),
                pltpu.VMEM(courant_lon.shape, f32),
                pltpu.VMEM(courant_lat.shape, f32),
                pltpu.VMEM((spec * rows, cols), f32),
                pltpu.VMEM(region_id.shape, jnp.int32),
                pltpu.VMEM(stiffness.shape, jnp.int32),
                pltpu.VMEM((spec * lev, spec), f32),
                pltpu.VMEM(inverses.shape, bf16),
                held, held, halo, halo, halo, halo, halo, halo,
                pltpu.VMEM((LP, rows * spec, cols), f32),
                pltpu.VMEM((spec, rows * cols), f32),
                pltpu.VMEM((3, rows, 8, cols), f32),
                pltpu.VMEM((n_lon, lat8, spec), f32),
                pltpu.VMEM((n_lon, lat8, spec), f32),
                pltpu.VMEM((n_lat, 1, spec), f32),
                pltpu.VMEM((n_lat, 1, spec), f32),
                dma((per,)), dma((nwin,)), dma, dma((5,)),
                dma((4, units)), dma((4, units)),
                dma((n_lon,)), dma((n_lon,)), dma((n_lat,)), dma((n_lat,)),
            ],
            compiler_params=pltpu.CompilerParams(collective_id=0, has_side_effects=True),
        )(
            adjoint_in.reshape(lev, spec * rows, cols),
            state.reshape(nwin, lev, spec * rows, cols),
            inverses.transpose(0, 2, 1, 3).reshape(steps, spec * lev, spec), courant_lon, courant_lat,
            emission.reshape(spec * rows, cols), region_id, stiffness,
        )
        out, grad = pl.pallas_call(
            finish,
            out_shape=(
                jax.ShapeDtypeStruct(out.shape, bf16),
                jax.ShapeDtypeStruct(grad.shape, f32),
            ),
            in_specs=[any_space] * 2,
            out_specs=(any_space, any_space),
            scratch_shapes=[dma((2,))],
        )(*(pltpu.with_memory_space_constraint(x, pltpu.VMEM) for x in (out, grad)))
        return out.reshape(adjoint_in.shape), grad

    in_specs = (
        P(None, None, "lat", "lon"),
        P(None, None, None, "lat", "lon"),
        P(),
        P("lat", "lon"),
        P("lat", "lon"),
        P(None, "lat", "lon"),
        P("lat", "lon"),
        P(None, "lat", "lon"),
    )
    out_specs = (P(None, None, "lat", "lon"), P(("lat", "lon"), None))
    return jax.shard_map(
        per_device, mesh=mesh, in_specs=in_specs, out_specs=out_specs, check_vma=False
    )
```

```python
import functools

import jax
import jax.numpy as jnp
from jax import lax
from jax.experimental import pallas as pl
from jax.experimental.pallas import tpu as pltpu
from jax.sharding import PartitionSpec as P

MESH = pl.DeviceIdType.MESH
LP = 2
AHEAD = 2


def kernel(
    n_lat, n_lon,
    adj_hbm, state_hbm, inv_hbm, clon_hbm, clat_hbm, em_hbm, reg_hbm, stiff_hbm,
    outbuf, grad_ref,
    adj, state, inv, clon_ref, clat_ref, em_ref, reg_ref, stiff_ref, tall, mats, lam_a, lam_b, west1, west2, south1, south2, east1, east2,
    tmp, fin, coef, part, inbox1, turn, inbox2,
    adj_sem, state_sem, inv_sem, small_sem, send_sem, recv_sem, s1, r1, s2, r2,
):
    lev, rows2, cols = adj.shape
    nwin = state.shape[0]
    steps = inv.shape[0]
    spec = rows2 // 2
    per = lev // LP
    units = nwin * per
    lat, lon = lax.axis_index("lat"), lax.axis_index("lon")
    north = jnp.maximum(lat - 1, 0)
    west = lax.rem(lon + n_lon - 1, n_lon)
    has_north = lat > 0
    has_south = lat < n_lat - 1

    barrier = pltpu.get_barrier_semaphore()
    for k in range(1, n_lon):
        pl.semaphore_signal(barrier, inc=1, device_id=(lat, lax.rem(lon + k, n_lon)), device_id_type=MESH)
    for k in range(1, n_lat):
        pl.semaphore_signal(barrier, inc=1, device_id=(lax.rem(lat + k, n_lat), lon), device_id_type=MESH)

    adj_loads = [
        pltpu.make_async_copy(
            adj_hbm.at[pl.ds(u * LP, LP)], adj.at[pl.ds(u * LP, LP)], adj_sem.at[u])
        for u in range(per)
    ]
    for load in adj_loads:
        load.start()
    inv_load = pltpu.make_async_copy(inv_hbm, inv, inv_sem)
    inv_load.start()
    small = [
        pltpu.make_async_copy(src, dst, small_sem.at[n])
        for n, (src, dst) in enumerate((
            (clon_hbm, clon_ref), (clat_hbm, clat_ref), (stiff_hbm, stiff_ref),
            (reg_hbm, reg_ref), (em_hbm, em_ref)))
    ]
    for load in small:
        load.start()
    state_loads = [
        pltpu.make_async_copy(state_hbm.at[w], state.at[w], state_sem.at[w]) for w in range(nwin)
    ]
    for w in reversed(range(nwin)):
        state_loads[w].start()

    lane = lax.broadcasted_iota(jnp.int32, (spec, cols), 1)

    def weights(r):
        return coef[0, r, 0:1, :], coef[1, r, 0:1, :], coef[2, r, 0:1, :]

    def remote(kind, src, dst, u, device):
        return pltpu.make_async_remote_copy(
            src_ref=src.at[u], dst_ref=dst.at[u],
            send_sem=send_sem.at[kind, u], recv_sem=recv_sem.at[kind, u],
            device_id=device, device_id_type=MESH,
        )

    def row_copy(kind, u):
        src, dst = ((lam_a, south1), (lam_b, south2))[kind]
        return remote(kind, src.at[0], dst, u, (north, lon))

    def col_copy(kind, u):
        src, dst = ((west1, east1), (west2, east2))[kind]
        return remote(kind + 2, src, dst, u, (lat, west))

    def pack(row0, row1):
        return jnp.where(lane == 0, row0, pltpu.roll(row1, 1, 1))

    def shift(row0, row1, edge):
        right0 = pltpu.roll(jnp.where(lane == 0, edge, row0), cols - 1, 1)
        right1 = pltpu.roll(jnp.where(lane == 0, pltpu.roll(edge, cols - 1, 1), row1), cols - 1, 1)
        return right0, right1

    def launch(u):
        @pl.when(has_north)
        def _():
            row_copy(0, u).start()
        for p in range(LP):
            west1[u, p] = pack(lam_a[0, u, p], lam_a[1, u, p])
        col_copy(0, u).start()

    def first_step(u):
        col_copy(0, u).wait_recv()
        c0, a0, o0 = weights(0)
        c1, a1, o1 = weights(1)
        for p in range(LP):
            row0, row1 = lam_a[0, u, p], lam_a[1, u, p]
            right0, right1 = shift(row0, row1, east1[u, p])
            lam_b[0, u, p] = c0 * row0 + a0 * row1 + o0 * right0
            lam_b[1, u, p] = c1 * row1 + o1 * right1

        @pl.when(has_north)
        def _():
            row_copy(1, u).start()

        @pl.when(has_south)
        def _():
            row_copy(0, u).wait_recv()
        for p in range(LP):
            row1 = lam_b[1, u, p] + a1 * south1[u, p]
            lam_b[1, u, p] = row1
            west2[u, p] = pack(lam_b[0, u, p], row1)
        col_copy(1, u).start()

    def second_step(u):
        col_copy(1, u).wait_recv()

        @pl.when(has_south)
        def _():
            row_copy(1, u).wait_recv()
        c0, a0, o0 = weights(0)
        c1, a1, o1 = weights(1)
        window = nwin - 1 - u // per
        group = u % per
        flats, ys, lives = [], [], []
        for p in range(LP):
            level = group * LP + p
            row0, row1 = lam_b[0, u, p], lam_b[1, u, p]
            right0, right1 = shift(row0, row1, east2[u, p])
            new0 = c0 * row0 + a0 * row1 + o0 * right0
            new1 = c1 * row1 + a1 * south2[u, p] + o1 * right1
            flats.append(jnp.concatenate([new0, new1], axis=1))
            tmp[p] = state[window, level].astype(jnp.float32)
            ys.append(jnp.concatenate(
                [tmp[p, pl.ds(0, spec, stride=2), :], tmp[p, pl.ds(1, spec, stride=2), :]], axis=1))
            live = stiff_ref[level]
            lives.append(jnp.concatenate([live[0:1], live[1:2]], axis=1))
        for s in reversed(range(steps)):
            mat = [mats[s, group * LP + p] for p in range(LP)]
            v1 = [jnp.dot(mat[p], flats[p].astype(jnp.bfloat16), preferred_element_type=jnp.float32) for p in range(LP)]
            v2 = [jnp.dot(mat[p], (v1[p] * ys[p]).astype(jnp.bfloat16), preferred_element_type=jnp.float32) for p in range(LP)]
            v3 = [jnp.dot(mat[p], (v2[p] * ys[p]).astype(jnp.bfloat16), preferred_element_type=jnp.float32) for p in range(LP)]
            flats = [
                jnp.where(lives[p] > s, 0.4 * flats[p] + 0.3 * v1[p] + 0.2 * v2[p] + 0.1 * v3[p], flats[p])
                for p in range(LP)
            ]
        return flats

    def store(u, flats):
        @pl.when(u < units - per)
        def _():
            for p in range(LP):
                for r in range(2):
                    lam_a[r, u + per, p] = flats[p][:, r * cols:(r + 1) * cols]
            launch(u + per)

        @pl.when(u >= units - per)
        def _():
            group = u - (units - per)
            for p in range(LP):
                for r in range(2):
                    tmp[p, pl.ds(r, spec, stride=2), :] = flats[p][:, r * cols:(r + 1) * cols]
                outbuf[group, p] = tmp[p].astype(jnp.bfloat16)

    def spread(k):
        to = lax.rem(lon + k, n_lon)
        return pltpu.make_async_remote_copy(
            src_ref=part.at[to], dst_ref=inbox1.at[lon], send_sem=s1.at[k], recv_sem=r1.at[lon],
            device_id=(lat, to), device_id_type=MESH)

    def spread_in(k):
        source = lax.rem(lon + k, n_lon)
        return source, pltpu.make_async_remote_copy(
            src_ref=part.at[source], dst_ref=inbox1.at[source], send_sem=s1.at[k], recv_sem=r1.at[source],
            device_id=(lat, source), device_id_type=MESH)

    def spread2(k):
        to = lax.rem(lat + k, n_lat)
        return pltpu.make_async_remote_copy(
            src_ref=turn.at[to], dst_ref=inbox2.at[lat], send_sem=s2.at[k], recv_sem=r2.at[lat],
            device_id=(to, lon), device_id_type=MESH)

    def spread2_in(k):
        source = lax.rem(lat + k, n_lat)
        return source, pltpu.make_async_remote_copy(
            src_ref=turn.at[source], dst_ref=inbox2.at[source], send_sem=s2.at[k], recv_sem=r2.at[source],
            device_id=(source, lon), device_id_type=MESH)

    def regions():
        lat8 = part.shape[1]
        contrib = jnp.concatenate([
            em_ref[pl.ds(r, spec, stride=2), :]
            * (lam_a[r, units - per, 0] + fin[:, r * cols:(r + 1) * cols])
            for r in range(2)], axis=1)
        where_from = jnp.concatenate([reg_ref[0:1, :], reg_ref[1:2, :]], axis=1)
        shape = (n_lon * lat8, 2 * cols)
        column = jnp.concatenate([jnp.full((lat8, 2 * cols), c, jnp.int32) for c in range(n_lon)], axis=0)
        band = lax.broadcasted_iota(jnp.int32, (lat8, 2 * cols), 0)
        band = jnp.concatenate([band] * n_lon, axis=0)
        onehot = (jnp.broadcast_to(where_from, shape) == band * n_lon + column).astype(jnp.float32)
        sums = lax.dot_general(
            onehot, contrib, (((1,), (1,)), ((), ())),
            precision=lax.Precision.HIGHEST, preferred_element_type=jnp.float32)
        for c in range(n_lon):
            part[c] = sums[c * lat8:(c + 1) * lat8]
        for k in range(1, n_lon):
            spread(k).start()

    def regions_turn():
        total = part[lon]
        for k in range(1, n_lon):
            source, copy = spread_in(k)
            copy.wait_recv()
            total = total + inbox1[source]
        for b in range(n_lat):
            turn[b] = total[b:b + 1]
        for k in range(1, n_lat):
            spread2(k).start()

    def regions_end():
        total = turn[lat]
        for k in range(1, n_lat):
            source, copy = spread2_in(k)
            copy.wait_recv()
            total = total + inbox2[source]
        grad_ref[...] = total

    def take(u):
        adj_loads[u].wait()
        for p in range(LP):
            tmp[p] = adj[u * LP + p].astype(jnp.float32)
            for r in range(2):
                lam_a[r, u, p] = tmp[p, pl.ds(r, spec, stride=2), :]

    take(0)
    pl.semaphore_wait(barrier, n_lon - 1 + n_lat - 1)
    launch(0)
    for u in range(1, AHEAD + 1):
        take(u)
        launch(u)

    @pl.when(jnp.logical_not(has_south))
    def _():
        south1[...] = jnp.zeros_like(south1)
        south2[...] = jnp.zeros_like(south2)

    for load in small:
        load.wait()
    for r in range(2):
        clon, clat = clon_ref[r:r + 1, :], clat_ref[r:r + 1, :]
        coef[0, r] = jnp.broadcast_to(1.0 - clon - clat, (8, cols))
        coef[1, r] = jnp.broadcast_to(clat, (8, cols))
        coef[2, r] = jnp.broadcast_to(clon, (8, cols))

    first_step(0)
    for u in range(AHEAD + 1, per):
        take(u)
    inv_load.wait()
    for s in range(steps):
        tall[...] = inv[s].astype(jnp.float32)
        for level in range(lev):
            mats[s, level] = tall[pl.ds(level, spec, stride=lev), :].T.astype(jnp.bfloat16)
    for u in range(1, AHEAD):
        first_step(u)
    for w in range(nwin):
        state_loads[w].wait()

    def body(u, carry):
        @pl.when(u + AHEAD + 1 < per)
        def _():
            launch(u + AHEAD + 1)

        @pl.when(u + AHEAD < units)
        def _():
            first_step(u + AHEAD)
        flats = second_step(u)
        store(u, flats)

        @pl.when(u == units - per)
        def _():
            fin[...] = flats[0]
            regions()

        @pl.when(u == units - per + 1)
        def _():
            regions_turn()
        return carry

    lax.fori_loop(0, units, body, 0)
    regions_end()

    def drain(u, carry):
        @pl.when(has_north)
        def _():
            row_copy(0, u).wait_send()
            row_copy(1, u).wait_send()
        col_copy(0, u).wait_send()
        col_copy(1, u).wait_send()
        return carry

    lax.fori_loop(0, units, drain, 0)
    for k in range(1, n_lon):
        spread(k).wait_send()
    for k in range(1, n_lat):
        spread2(k).wait_send()


def finish(held_ref, grad_ref, out_hbm, grad_hbm, sems):
    copies = [
        pltpu.make_async_copy(held_ref, out_hbm, sems.at[0]),
        pltpu.make_async_copy(grad_ref, grad_hbm, sems.at[1]),
    ]
    for copy in copies:
        copy.start()
    for copy in copies:
        copy.wait()


def solution(mesh):
    n_lat, n_lon = mesh.shape["lat"], mesh.shape["lon"]

    def per_device(adjoint_in, state, inverses, courant_lon, courant_lat, emission, region_id, stiffness):
        lev, spec, rows, cols = adjoint_in.shape
        nwin, steps = state.shape[0], inverses.shape[0]
        per = lev // LP
        units = nwin * per
        lat8 = -(-n_lat // 8) * 8
        f32, bf16 = jnp.float32, jnp.bfloat16
        any_space = pl.BlockSpec(memory_space=pl.ANY)
        vmem = pl.BlockSpec(memory_space=pltpu.VMEM)
        halo = pltpu.VMEM((units, LP, spec, cols), f32)
        held = pltpu.VMEM((2, units, LP, spec, cols), f32)
        dma = pltpu.SemaphoreType.DMA
        out, grad = pl.pallas_call(
            functools.partial(kernel, n_lat, n_lon),
            out_shape=(
                pltpu.VMEM((per, LP, rows * spec, cols), bf16),
                pltpu.VMEM((1, spec), f32),
            ),
            in_specs=[any_space] * 8,
            out_specs=(vmem, vmem),
            scratch_shapes=[
                pltpu.VMEM((lev, rows * spec, cols), bf16),
                pltpu.VMEM((nwin, lev, rows * spec, cols), bf16),
                pltpu.VMEM((steps, spec * lev, spec), bf16),
                pltpu.VMEM(courant_lon.shape, f32),
                pltpu.VMEM(courant_lat.shape, f32),
                pltpu.VMEM((spec * rows, cols), f32),
                pltpu.VMEM(region_id.shape, jnp.int32),
                pltpu.VMEM(stiffness.shape, jnp.int32),
                pltpu.VMEM((spec * lev, spec), f32),
                pltpu.VMEM(inverses.shape, bf16),
                held, held, halo, halo, halo, halo, halo, halo,
                pltpu.VMEM((LP, rows * spec, cols), f32),
                pltpu.VMEM((spec, rows * cols), f32),
                pltpu.VMEM((3, rows, 8, cols), f32),
                pltpu.VMEM((n_lon, lat8, spec), f32),
                pltpu.VMEM((n_lon, lat8, spec), f32),
                pltpu.VMEM((n_lat, 1, spec), f32),
                pltpu.VMEM((n_lat, 1, spec), f32),
                dma((per,)), dma((nwin,)), dma, dma((5,)),
                dma((4, units)), dma((4, units)),
                dma((n_lon,)), dma((n_lon,)), dma((n_lat,)), dma((n_lat,)),
            ],
            compiler_params=pltpu.CompilerParams(collective_id=0, has_side_effects=True),
        )(
            adjoint_in.reshape(lev, spec * rows, cols),
            state.reshape(nwin, lev, spec * rows, cols),
            inverses.transpose(0, 2, 1, 3).reshape(steps, spec * lev, spec), courant_lon, courant_lat,
            emission.reshape(spec * rows, cols), region_id, stiffness,
        )
        out, grad = pl.pallas_call(
            finish,
            out_shape=(
                jax.ShapeDtypeStruct(out.shape, bf16),
                jax.ShapeDtypeStruct(grad.shape, f32),
            ),
            in_specs=[any_space] * 2,
            out_specs=(any_space, any_space),
            scratch_shapes=[dma((2,))],
        )(*(pltpu.with_memory_space_constraint(x, pltpu.VMEM) for x in (out, grad)))
        return out.reshape(adjoint_in.shape), grad

    in_specs = (
        P(None, None, "lat", "lon"),
        P(None, None, None, "lat", "lon"),
        P(),
        P("lat", "lon"),
        P("lat", "lon"),
        P(None, "lat", "lon"),
        P("lat", "lon"),
        P(None, "lat", "lon"),
    )
    out_specs = (P(None, None, "lat", "lon"), P(("lat", "lon"), None))
    return jax.shard_map(
        per_device, mesh=mesh, in_specs=in_specs, out_specs=out_specs, check_vma=False
    )
```
